32 devices in a mesh: head: 4 (over y, x), seq: 8 (over z, core).
Axes of the slice: x: 2, y: 2, z: 4, core: 2. Of those that a mesh axis runs over, the one named last changes fastest.
Arguments:
- queries: bfloat16 [8, 16, 32, 128], P(None, None, 'head'), may hold values from -4000 to 4000
- cache_keys: bfloat16 [16, 16, 1024, 128], P(None, 'head', 'seq'), may hold values from -6 to 6
- stored_values: bfloat16 [16, 16, 1024, 128], P(None, 'head', 'seq'), may hold values from -6 to 6
- new_keys: bfloat16 [8, 16, 16, 128], P(None, None, 'head'), may hold values from -12 to 12
- decoded_values: bfloat16 [8, 16, 16, 128], P(None, None, 'head'), may hold values from -6 to 6
- keep_mask: int32 [16, 1024], P(None, 'seq'), may hold values from 0 to 1
Outputs:
- attended: bfloat16 [8, 16, 4096], P(None, None, 'head')
- importance: float32 [16, 1024], P('head', 'seq')
The draws below stay inside these ranges and needn't reach their ends.
All inputs are finite; a program needn't handle non-finite values.
Results may differ from the reference program's by a relative error of at most 0.0034.
Values sent between devices are 32-bit elements; how exact they have to be, the bound alone decides.
No kernel may reach another device: no remote copies, remote signals or barrier semaphores. Data moves between devices by JAX's collectives and lax.ppermute only.
A program may use at most 128 MiB of HBM per device.

```python
import jax
import jax.numpy as jnp
from jax import lax

HQ = 32
KEY_VALUE_HEADS = 16
HEAD_SIZE = 128
BATCH_SEQUENCES = 16
BLOCK_TOKENS = 128
DECODE_STEPS = 8
CONTEXT_TOKENS = 1024


def base_queries(key):
    return jax.random.truncated_normal(jax.random.fold_in(key, 31), -6.0, 6.0, (DECODE_STEPS, BATCH_SEQUENCES, HQ, HEAD_SIZE), jnp.float32)


def chosen_positions(key):
    first_pos = jax.random.randint(jax.random.fold_in(key, 51), (BATCH_SEQUENCES,), 0, CONTEXT_TOKENS)
    second_pos = (first_pos + CONTEXT_TOKENS // 2) % CONTEXT_TOKENS
    return (first_pos, second_pos)


def drawn_keys(key):
    key_rows = jax.random.truncated_normal(jax.random.fold_in(key, 41), -6.0, 6.0, (BATCH_SEQUENCES, KEY_VALUE_HEADS, CONTEXT_TOKENS, HEAD_SIZE), jnp.float32)
    return key_rows


def draw_cache_keys(key, part):
    key_rows = drawn_keys(key)
    return key_rows.astype(jnp.bfloat16)


def draw_queries(key, part):
    query_rows = base_queries(key)
    return query_rows.astype(jnp.bfloat16)


def draw_new_keys(key, part):
    query_rows = base_queries(key)
    paired = query_rows[:, :, 0::2, :] + query_rows[:, :, 1::2, :]
    random_jitter = jax.random.truncated_normal(jax.random.fold_in(key, 71), -6.0, 6.0, (DECODE_STEPS, BATCH_SEQUENCES, KEY_VALUE_HEADS, HEAD_SIZE), jnp.float32)
    return (0.7 * paired + 0.5 * random_jitter).astype(jnp.bfloat16)


def draw_keep_mask(key, part):
    kept = jax.random.randint(jax.random.fold_in(key, 81), (BATCH_SEQUENCES, CONTEXT_TOKENS), 0, 4) > 0
    first_pos, second_pos = chosen_positions(key)
    places = jnp.arange(CONTEXT_TOKENS)[None, :]
    forced = (places == first_pos[:, None]) | (places == second_pos[:, None])
    return (kept | forced).astype(jnp.int32)


def steps_of(own_key, extent, split, low, largest):
    factor_of, own = 1.0, jax.random.fold_in(own_key, 6)
    for position, parts in split:
        draws = jnp.exp(jax.random.uniform(jax.random.fold_in(own, position), (parts,), jnp.float32, low / len(split), largest / len(split)))
        factor_of = factor_of * jnp.repeat(draws, extent[position] // parts).reshape([-1 if axis == position else 1 for axis in range(len(extent))])
    return factor_of


def bell_draw(key, extent, width, most, split=(), dtype=jnp.bfloat16):
    array = jax.random.normal(key, extent, jnp.float32) * width
    if len(split) > 0:
        array = steps_of(key, extent, split, -0.22, 0.18) * array
    return jnp.clip(array, min=-most, max=most).astype(dtype)


def setup_inputs(seed: int = 0) -> dict:
    streams_of = jax.random.split(jax.random.key(seed), 7)
    return {
        "queries": draw_queries(jax.random.fold_in(streams_of[6], 71), 0),
        "cache_keys": draw_cache_keys(jax.random.fold_in(streams_of[6], 71), 0),
        "stored_values": bell_draw(streams_of[2], (BATCH_SEQUENCES, KEY_VALUE_HEADS, CONTEXT_TOKENS, HEAD_SIZE), 1.0, 6.0, ((1, 4), (2, 8))),
        "new_keys": draw_new_keys(jax.random.fold_in(streams_of[6], 71), 0),
        "decoded_values": bell_draw(streams_of[4], (DECODE_STEPS, BATCH_SEQUENCES, KEY_VALUE_HEADS, HEAD_SIZE), 1.0, 6.0, ((2, 4),)),
        "keep_mask": draw_keep_mask(jax.random.fold_in(streams_of[6], 71), 0),
    }


score_scale = 1.0 / 12.0
far_below = -1e30


def one_row(inputs):
    query_rows, key_cache, value_store_cache, fresh_keys, fresh_values, kept_row = inputs
    block_count = CONTEXT_TOKENS // BLOCK_TOKENS
    grouped_queries = query_rows.astype(jnp.float32).reshape(DECODE_STEPS, KEY_VALUE_HEADS, 2, HEAD_SIZE)
    logit_scores = jnp.einsum('thgd,hsd->thgs', grouped_queries, key_cache.astype(jnp.float32)) * score_scale
    scores_per_block = logit_scores.reshape(DECODE_STEPS, KEY_VALUE_HEADS, 2, block_count, BLOCK_TOKENS)
    block_keep = (kept_row > 0).reshape(block_count, BLOCK_TOKENS)
    block_peak = jnp.max(jnp.where(block_keep, scores_per_block, far_below), axis=-1)
    block_exp = jnp.where(block_keep, jnp.exp(scores_per_block - block_peak[..., None]), 0.0)
    block_total = jnp.sum(block_exp, axis=-1)
    block_weights = lax.optimization_barrier(block_exp.astype(jnp.bfloat16)).astype(jnp.float32)
    blocked_values = value_store_cache.astype(jnp.float32).reshape(KEY_VALUE_HEADS, block_count, BLOCK_TOKENS, HEAD_SIZE)
    block_sum = jnp.einsum('thgks,hksd->thgkd', block_weights, blocked_values)
    new_scores = jnp.einsum('thgd,jhd->thgj', grouped_queries, fresh_keys.astype(jnp.float32)) * score_scale
    causal = (jnp.arange(DECODE_STEPS)[None, :] <= jnp.arange(DECODE_STEPS)[:, None])[:, None, None, :]
    new_peak = jnp.max(jnp.where(causal, new_scores, far_below), axis=-1)
    new_exp = jnp.where(causal, jnp.exp(new_scores - new_peak[..., None]), 0.0)
    new_total = jnp.sum(new_exp, axis=-1)
    new_weights = lax.optimization_barrier(new_exp.astype(jnp.bfloat16)).astype(jnp.float32)
    new_sum = jnp.einsum('thgj,jhd->thgd', new_weights, fresh_values.astype(jnp.float32))
    peak = jnp.maximum(jnp.max(block_peak, axis=-1), new_peak)
    block_factor = jnp.exp(block_peak - peak[..., None])
    new_factor = jnp.exp(new_peak - peak)
    total = jnp.sum(block_total * block_factor, axis=-1) + new_total * new_factor
    weighted = jnp.sum(block_sum * block_factor[..., None], axis=3) + new_sum * new_factor[..., None]
    attended = (weighted / total[..., None]).astype(jnp.bfloat16).reshape(DECODE_STEPS, HQ * HEAD_SIZE)
    kept = (kept_row > 0)[None, None, None, :]
    shares = jnp.where(kept, jnp.exp(logit_scores - peak[..., None]), 0.0) / total[..., None]
    importance = jnp.sum(shares, axis=(0, 1, 2)) * (CONTEXT_TOKENS / (DECODE_STEPS * HQ))
    return attended, importance


def reference(queries, cache_keys, stored_values, new_keys, decoded_values, keep_mask):
    inputs = (jnp.swapaxes(queries, 0, 1), cache_keys, stored_values,
              jnp.swapaxes(new_keys, 0, 1), jnp.swapaxes(decoded_values, 0, 1), keep_mask)
    attended, importance = lax.map(one_row, inputs)
    return jnp.swapaxes(attended, 0, 1), importance
```

```python
import functools
import math

import jax
import jax.numpy as jnp
from jax import lax
from jax.experimental import pallas as pl
from jax.experimental.pallas import tpu as pltpu
from jax.sharding import PartitionSpec as P

HQ = 32
DECODE_STEPS = 8

SCORE_SCALE = 1.0 / 12.0
FAR_BELOW = -1e30
LANES = 128
SUBLANES = 8


VMEM = pl.BlockSpec(memory_space=pltpu.VMEM)


def digits_of(count):
    sizes, left = [], count
    while left > 1:
        size = 2 if not sizes else min(4, left)
        assert left % size == 0
        sizes.append(size)
        left //= size
    return sizes


def digit(index, sizes, stage):
    return lax.rem(index // math.prod(sizes[:stage]), sizes[stage])


def exchange(array, axis, sizes, stage, k):
    count, step = math.prod(sizes), math.prod(sizes[:stage])
    return lax.ppermute(array, axis, [(i, i ^ (k * step)) for i in range(count)])


def lane_ids(rows):
    return lax.broadcasted_iota(jnp.int32, (rows, LANES), 1)


def pack_stats(stats, batch, units):
    rows = units * SUBLANES
    used = 2 * batch
    kept = jnp.where(lane_ids(stats.shape[0]) < used, stats, 0.0)
    packed = kept[:rows]
    for g in range(1, stats.shape[0] // rows):
        packed = packed + pltpu.roll(kept[g * rows : (g + 1) * rows], g * used, 1)
    return packed.reshape(units, SUBLANES, LANES)


def unpack_stats(packed, batch, rows):
    used = 2 * batch
    flat = packed.reshape(packed.shape[0] * SUBLANES, LANES)
    groups = [flat]
    for g in range(1, rows // flat.shape[0]):
        groups.append(pltpu.roll(flat, LANES - g * used, 1))
    return jnp.concatenate(groups, axis=0)


def merge_stats(parts, batch):
    peak = functools.reduce(jnp.maximum, parts)
    low = lane_ids(peak.shape[0]) < batch
    factors = [jnp.where(low, jnp.exp(jnp.where(low, part - peak, 0.0)), 0.0) for part in parts]
    total = sum(part * pltpu.roll(factor, batch, 1) for part, factor in zip(parts, factors))
    return jnp.where(low, peak, total), factors


def column(block, lane):
    if isinstance(lane, int):
        return jnp.broadcast_to(block[:, lane : lane + 1], block.shape)
    chosen = jnp.where(lane_ids(block.shape[0]) == lane, block, 0.0)
    return jnp.broadcast_to(jnp.sum(chosen, axis=1, keepdims=True), block.shape)


def by_group(products, shape, group_of_row):
    out = products[0]
    for g in range(1, len(products)):
        out = jnp.where(group_of_row == g, products[g], out)
    return out


def local_kernel(sizes, per_step, q_ref, k_ref, v_ref, mask_ref, own_ref, send_ref, e_ref, stats_ref):
    step = pl.program_id(0)
    steps, batch_here, heads, width = q_ref.shape
    kv, positions = k_ref.shape[1], k_ref.shape[2]
    rows = steps * heads
    batch = per_step * pl.num_programs(0) if isinstance(pl.num_programs(0), int) else None
    batch = mask_ref.shape[0]
    half = own_ref.shape[0] - stats_units(rows, batch)
    core = digit(lax.axis_index("seq"), sizes, 0)
    group_of_row = lax.rem(lax.broadcasted_iota(jnp.int32, (rows, 1), 0), heads) // (heads // kv)
    lanes = lane_ids(rows)

    @pl.when(step == 0)
    def _():
        stats_ref[...] = jnp.zeros_like(stats_ref)

    stats = stats_ref[...]
    for i in range(per_step):
        b = step * per_step + i
        q = q_ref[:, i].astype(jnp.float32).reshape(rows, width).astype(jnp.bfloat16)
        k = k_ref[i].reshape(kv * positions, width)
        scores = lax.dot_general(q, k, (((1,), (1,)), ((), ())), preferred_element_type=jnp.float32)
        scores = by_group(
            [scores[:, g * positions : (g + 1) * positions] for g in range(kv)], None, group_of_row
        )
        keep = mask_ref[pl.ds(b, 1), :] > 0
        scores = jnp.where(keep, scores * SCORE_SCALE, FAR_BELOW)
        peak = jnp.max(scores, axis=1, keepdims=True)
        e = jnp.where(keep, jnp.exp(scores - peak), 0.0)
        total = jnp.sum(e, axis=1, keepdims=True)
        e_ref[i] = e
        weights = e.astype(jnp.bfloat16)
        out = by_group(
            [jnp.dot(weights, v_ref[i, g], preferred_element_type=jnp.float32) for g in range(kv)],
            None,
            group_of_row,
        ).reshape(steps, heads, width)
        stats = jnp.where(lanes == b, peak, stats)
        stats = jnp.where(lanes == b + batch, total, stats)
        for t in range(steps // 2):
            first, second = out[t], out[t + steps // 2]
            own_ref[t * batch + b] = jnp.where(core == 0, first, second)
            send_ref[t * batch + b] = jnp.where(core == 0, second, first)
    stats_ref[...] = stats

    @pl.when(step == pl.num_programs(0) - 1)
    def _():
        packed = pack_stats(stats, batch, stats_units(rows, batch))
        own_ref[half:] = packed
        send_ref[half:] = packed


def stats_units(rows, batch):
    return rows * 2 * batch // LANES // SUBLANES


def unit_base(index, sizes, stage, units):
    base, left = 0, units
    for s in range(stage):
        left //= sizes[s]
        base = base + digit(index, sizes, s) * left
    return base, left


def combine_kernel(sizes, stage, units, batch, *refs):
    came, fanout = sizes[stage - 1], sizes[stage]
    ins, outs, scratch = refs[:came], refs[came : came + fanout], refs[came + fanout :]
    packed_units = outs[0].shape[0] - ins[0].shape[0] + (ins[0].shape[0] - outs[0].shape[0])
    extra = stats_units(scratch[0].shape[0], batch)
    rows = scratch[0].shape[0]
    index = lax.axis_index("seq")
    base, kept = unit_base(index, sizes, stage, units)
    part = kept // fanout
    parts = [unpack_stats(ref[kept:], batch, rows) for ref in ins]
    merged, factors = merge_stats(parts, batch)
    for ref, factor in zip(scratch, factors):
        ref[...] = factor
    packed = pack_stats(merged, batch, extra)
    me = digit(index, sizes, stage)
    for k in range(fanout):
        start = lax.bitwise_xor(me, k) * part
        for j in range(part):
            factor_blocks = unit_factors(scratch, base + start, j, batch, part)
            outs[k][j] = sum(ref[start + j] * factor for ref, factor in zip(ins, factor_blocks))
        outs[k][part:] = packed


def unit_factors(refs, first, j, batch, part):
    if part % batch == 0:
        row = (first // batch + j // batch) * SUBLANES
        lane = j % batch
    else:
        row = ((first + j) // batch) * SUBLANES
        lane = lax.rem(first + j, batch)
    return [column(ref[pl.ds(pl.multiple_of(row, SUBLANES), SUBLANES), :], lane) for ref in refs]


def new_kernel(q_ref, nk_ref, nv_ref, out_ref, stats_ref):
    steps, batch, heads, width = q_ref.shape
    kv, fresh = nk_ref.shape[1], nk_ref.shape[2]
    rows = steps * heads
    row = lax.broadcasted_iota(jnp.int32, (rows, kv * fresh), 0)
    col = lax.broadcasted_iota(jnp.int32, (rows, kv * fresh), 1)
    seen = (lax.rem(row, heads) // (heads // kv) == col // fresh) & (lax.rem(col, fresh) <= row // heads)
    lanes = lane_ids(rows)
    stats = jnp.zeros((rows, LANES), jnp.float32)
    for b in range(batch):
        q = q_ref[:, b].astype(jnp.float32).reshape(rows, width).astype(jnp.bfloat16)
        nk = nk_ref[b].astype(jnp.float32).reshape(kv * fresh, width).astype(jnp.bfloat16)
        nv = nv_ref[b].astype(jnp.float32).reshape(kv * fresh, width).astype(jnp.bfloat16)
        scores = lax.dot_general(q, nk, (((1,), (1,)), ((), ())), preferred_element_type=jnp.float32)
        scores = jnp.where(seen, scores * SCORE_SCALE, FAR_BELOW)
        peak = jnp.max(scores, axis=1, keepdims=True)
        e = jnp.where(seen, jnp.exp(scores - peak), 0.0)
        total = jnp.sum(e, axis=1, keepdims=True)
        out = jnp.dot(e.astype(jnp.bfloat16), nv, preferred_element_type=jnp.float32)
        out = out.reshape(steps, heads, width)
        for t in range(steps):
            out_ref[t * batch + b] = out[t]
        stats = jnp.where(lanes == b, peak, stats)
        stats = jnp.where(lanes == b + batch, total, stats)
    stats_ref[...] = stats


def finish_kernel(sizes, units, batch, *refs):
    came = sizes[-1]
    ins, new_out, new_stats, own_stats = refs[:came], refs[came], refs[came + 1], refs[came + 2]
    attended, shares = refs[came + 3], refs[came + 4]
    scratch = refs[came + 5 :]
    rows = new_stats.shape[0]
    index = lax.axis_index("seq")
    base, kept = unit_base(index, sizes, len(sizes), units)
    parts = [unpack_stats(ref[kept:], batch, rows) for ref in ins] + [new_stats[...]]
    merged, factors = merge_stats(parts, batch)
    low = lane_ids(rows) < batch
    inverse = 1.0 / jnp.where(low, pltpu.roll(merged, LANES - batch, 1), 1.0)
    for ref, factor in zip(scratch, factors):
        ref[...] = factor * inverse
    shares[...] = jnp.exp(jnp.where(low, own_stats[...] - merged, 0.0)) * inverse
    for j in range(kept):
        blocks = unit_factors(scratch, base, j, batch, kept)
        value = sum(ref[j] * block for ref, block in zip(ins, blocks)) + new_out[base + j] * blocks[-1]
        attended[j] = value.astype(jnp.bfloat16).astype(jnp.float32)


def importance_kernel(head_sizes, weight, e_ref, shares_ref, *refs):
    count = math.prod(head_sizes)
    outs, scratch = refs[:count], refs[count]
    batch, rows, positions = e_ref.shape
    each = batch // count
    shares = shares_ref[...] * weight
    for b in range(batch):
        value = jnp.sum(e_ref[b] * shares[:, b : b + 1], axis=0, keepdims=True)
        scratch[b // each, pl.ds(b % each, 1), :] = value
    me = lax.axis_index("head")
    for k in range(count):
        outs[k][...] = scratch[lax.bitwise_xor(me, k)][:each]


def assemble_kernel(sizes, masks, batch, heads, *refs):
    count = len(masks)
    pieces, imps = refs[:count], refs[count:-3]
    attended, importance, scratch = refs[-3:]
    index = lax.axis_index("seq")
    each = pieces[0].shape[0]
    for piece, mask in zip(pieces, masks):
        base, _ = unit_base(lax.bitwise_xor(index, mask), sizes, len(sizes), each * count)
        scratch[pl.ds(base * heads, each * heads), :] = piece[...].reshape(each * heads, LANES)
    for t in range(attended.shape[0]):
        for h in range(heads):
            rows = scratch[pl.ds(t * batch * heads + h, batch, stride=heads), :]
            attended[t, :, h * LANES : (h + 1) * LANES] = rows.astype(jnp.bfloat16)
    importance[...] = sum(ref[...] for ref in imps)


def shape_of(shape, dtype=jnp.float32):
    return jax.ShapeDtypeStruct(shape, dtype)


def call(kernel, outs, count_in, flops, name, scratch=()):
    return pl.pallas_call(
        kernel,
        out_shape=outs,
        in_specs=[VMEM] * count_in,
        out_specs=jax.tree.map(lambda _: VMEM, outs),
        scratch_shapes=list(scratch),
        cost_estimate=pl.CostEstimate(flops=flops, bytes_accessed=1 << 20, transcendentals=0),
        name=name,
    )


def on_device(queries, cache_keys, stored_values, new_keys, decoded_values, keep_mask):
    steps, batch, heads, width = queries.shape
    kv, positions = cache_keys.shape[1], cache_keys.shape[2]
    rows, units = steps * heads, steps * batch
    sizes = digits_of(lax.axis_size("seq"))
    head_count = lax.axis_size("head")
    weight = positions * lax.axis_size("seq") / (DECODE_STEPS * HQ)
    extra = stats_units(rows, batch)
    per_step = 4
    stats_block = (rows, LANES)

    half = (units // 2 + extra, SUBLANES, LANES)
    whole = lambda s: pl.BlockSpec(s, lambda i: (0,) * len(s))
    own, send, e, own_stats = pl.pallas_call(
        functools.partial(local_kernel, sizes, per_step),
        grid=(batch // per_step,),
        in_specs=[
            pl.BlockSpec((steps, per_step, heads, width), lambda i: (0, i, 0, 0)),
            pl.BlockSpec((per_step, kv, positions, width), lambda i: (i, 0, 0, 0)),
            pl.BlockSpec((per_step, kv, positions, width), lambda i: (i, 0, 0, 0)),
            whole((batch, positions)),
        ],
        out_specs=[
            whole(half),
            whole(half),
            pl.BlockSpec((per_step, rows, positions), lambda i: (i, 0, 0)),
            whole(stats_block),
        ],
        out_shape=[
            shape_of(half),
            shape_of(half),
            shape_of((batch, rows, positions)),
            shape_of(stats_block),
        ],
        cost_estimate=pl.CostEstimate(flops=1 << 28, bytes_accessed=1 << 22, transcendentals=0),
        name="local",
    )(queries, cache_keys, stored_values, keep_mask)

    new_out, new_stats = call(
        new_kernel, [shape_of((units, SUBLANES, LANES)), shape_of(stats_block)], 3, 1 << 24, "fresh"
    )(queries, jnp.transpose(new_keys, (1, 2, 0, 3)), jnp.transpose(decoded_values, (1, 2, 0, 3)))

    came, left = [own, exchange(send, "seq", sizes, 0, 1)], units // 2
    for stage in range(1, len(sizes)):
        left //= sizes[stage]
        outs = call(
            functools.partial(combine_kernel, sizes, stage, units, batch),
            [shape_of((left + extra, SUBLANES, LANES))] * sizes[stage],
            len(came),
            1 << 24,
            f"combine{stage}",
            [pltpu.VMEM(stats_block, jnp.float32)] * len(came),
        )(*came)
        came = [outs[0]] + [exchange(outs[k], "seq", sizes, stage, k) for k in range(1, sizes[stage])]

    attended, shares = call(
        functools.partial(finish_kernel, sizes, units, batch),
        [shape_of((left, SUBLANES, LANES)), shape_of(stats_block)],
        len(came) + 3,
        1 << 24,
        "finish",
        [pltpu.VMEM(stats_block, jnp.float32)] * (len(came) + 1),
    )(*came, new_out, new_stats, own_stats)

    pieces, masks = [attended], [0]
    for stage in reversed(range(len(sizes))):
        step = math.prod(sizes[:stage])
        more = [
            (exchange(piece, "seq", sizes, stage, k), mask ^ (k * step))
            for k in range(1, sizes[stage])
            for piece, mask in zip(pieces, masks)
        ]
        pieces, masks = pieces + [m[0] for m in more], masks + [m[1] for m in more]

    each = batch // head_count
    head_sizes = [head_count]
    imps = call(
        functools.partial(importance_kernel, head_sizes, weight),
        [shape_of((each, positions))] * head_count,
        2,
        1 << 24,
        "importance",
        [pltpu.VMEM((head_count, SUBLANES * -(-each // SUBLANES), positions), jnp.float32)],
    )(e, shares)
    imps = [imps[0]] + [exchange(imps[k], "head", head_sizes, 0, k) for k in range(1, head_count)]

    return call(
        functools.partial(assemble_kernel, sizes, masks, batch, heads),
        (shape_of((steps, batch, heads * width), jnp.bfloat16), shape_of((each, positions))),
        len(pieces) + len(imps),
        1 << 24,
        "assemble",
        [pltpu.VMEM((units * heads, LANES), jnp.float32)],
    )(*pieces, *imps)


def solution(mesh):
    return jax.shard_map(
        on_device,
        mesh=mesh,
        in_specs=(
            P(None, None, "head", None),
            P(None, "head", "seq", None),
            P(None, "head", "seq", None),
            P(None, None, "head", None),
            P(None, None, "head", None),
            P(None, "seq"),
        ),
        out_specs=(P(None, None, "head"), P("head", "seq")),
        check_vma=False,
    )
```
